32 devices in a mesh: tm: 8 (over z, y), row: 2 (over core), col: 2 (over x).
Axes of the slice: x: 2, y: 2, z: 4, core: 2. Of those that a mesh axis runs over, the one named last changes fastest.
Arguments:
- precision_diag: float32 [16, 512, 512], P('tm', 'row', 'col'), may hold values from -4 to 16, as said below
- precision_link: float32 [16, 512, 512], P('tm', 'row', 'col'), may hold values from -8 to 2
Outputs:
- pivots: float32 [16, 512, 512], P('tm', 'row', 'col')
- couplings: float32 [16, 512, 512], P('tm', 'row', 'col')
- log_variance: float32 [16, 512], P('tm', ('row', 'col'))
The draws below stay inside these ranges and needn't reach their ends.
Inputs may be any that keep to these rules, and one draw needn't show every extreme that they name: precision_diag and precision_link form a symmetric positive definite block-tridiagonal matrix as in the reference program.
All inputs are finite; a program needn't handle non-finite values.
Results may differ from the reference program's by a relative error of at most 0.0003.
Values sent between devices are 32-bit elements; how exact they have to be, the bound alone decides.
A program may use at most 128 MiB of HBM per device.

```python
import math
import jax
import jax.numpy as jnp
from jax import lax

NS = 512
LEVELS = 4
NT = 16


def paired_product(left_stack, right_stack):
    return jnp.einsum('jki,jkl->jil', left_stack, right_stack, precision=lax.Precision.HIGHEST)


def build_precision(key):
    base_key = jax.random.fold_in(key, 11)
    subkeys = jax.random.split(base_key, 6)
    scales = jnp.exp(jax.random.uniform(subkeys[0], (NT, NS), jnp.float32, math.log(0.7), math.log(2.2)))
    identity = jnp.eye(NS, dtype=jnp.float32)
    roughness = jax.random.normal(subkeys[1], (NT, NS, NS), jnp.float32) * (0.5 / math.sqrt(NS))
    factor = jnp.triu(roughness, 1) + scales[:, :, None] * identity
    persistence = jax.random.uniform(subkeys[2], (NT,), jnp.float32, 0.985, 0.999)
    shocked = jax.random.uniform(subkeys[3], (NT,), jnp.float32) < 0.03
    persistence = jnp.where(shocked, 0.6, persistence)
    perturbation = jax.random.normal(subkeys[4], (NT, NS, NS), jnp.float32) * (0.1 / math.sqrt(NS))
    transfer = persistence[:, None, None] * (factor + perturbation)
    nugget = jnp.exp(jax.random.uniform(subkeys[5], (NT, NS), jnp.float32, math.log(0.0001), math.log(0.01))) * scales * scales
    next_factor = jnp.roll(factor, -1, axis=0)
    next_transfer = jnp.roll(transfer, -1, axis=0)
    present = (jnp.arange(NT) < NT - 1).astype(jnp.float32)[:, None, None]
    diagonal_blocks = paired_product(factor, factor) + present * paired_product(next_transfer, next_transfer) + nugget[:, :, None] * identity
    link_blocks = -paired_product(next_factor, next_transfer)
    return (diagonal_blocks, link_blocks)


def draw_precision_diag(key, part):
    return build_precision(key)[0]


def draw_precision_link(key, part):
    return build_precision(key)[1]


def setup_inputs(seed: int = 0) -> dict:
    key_list = jax.random.split(jax.random.key(seed), 3)
    precision_diag = draw_precision_diag(jax.random.fold_in(key_list[2], 71), 0)
    precision_link = draw_precision_link(jax.random.fold_in(key_list[2], 71), 0)
    return dict(precision_diag=precision_diag, precision_link=precision_link)


def product_tn(left_part, right_part):
    return jnp.einsum('ki,kl->il', left_part, right_part, precision=lax.Precision.HIGHEST)

def eliminate_block(pivot, below_link, above_link):
    node_count = pivot.shape[0]
    lower_factor = jnp.linalg.cholesky(pivot)
    right_side = jnp.concatenate([below_link, above_link.T, jnp.eye(node_count, dtype=pivot.dtype)], axis=1)
    solved = jax.scipy.linalg.solve_triangular(lower_factor, right_side, lower=True)
    lower_panel = solved[:, :node_count]
    upper_panel = solved[:, node_count:2 * node_count]
    inverse_part = solved[:, 2 * node_count:]
    log_part = jnp.log(jnp.sum(inverse_part * inverse_part, axis=0))
    return (log_part, product_tn(lower_panel, lower_panel), product_tn(upper_panel, upper_panel), -product_tn(upper_panel, lower_panel))

def final_block(pivot):
    node_count = pivot.shape[0]
    lower_factor = jnp.linalg.cholesky(pivot)
    inverse_part = jax.scipy.linalg.solve_triangular(lower_factor, jnp.eye(node_count, dtype=pivot.dtype), lower=True)
    return jnp.log(jnp.sum(inverse_part * inverse_part, axis=0))

def reference(precision_diag, precision_link):
    block_total = precision_diag.shape[0]
    node_count = precision_diag.shape[1]
    pivots = precision_diag
    links = precision_link.at[block_total - 1].set(jnp.zeros((node_count, node_count), precision_link.dtype))
    out_pivots = pivots
    out_links = links
    out_logs = jnp.zeros((block_total, node_count), precision_diag.dtype)
    for level_num in range(LEVELS):
        stride = 2 ** level_num
        removed = jnp.arange(stride, block_total, 2 * stride, dtype=jnp.int32)
        lower_ids = (removed - stride).astype(jnp.int32)
        upper_ids = (removed + stride).astype(jnp.int32)
        log_part, gram_down, gram_up, link_new = jax.vmap(eliminate_block)(pivots[removed], links[lower_ids], links[removed])
        out_pivots = out_pivots.at[removed].set(pivots[removed])
        out_links = out_links.at[removed].set(links[removed])
        out_logs = out_logs.at[removed].set(log_part)
        pivots = pivots.at[lower_ids].add(-gram_down)
        pivots = pivots.at[upper_ids].add(-gram_up, mode='drop')
        links = links.at[lower_ids].set(link_new)
    kept = jnp.arange(0, block_total, 2 ** LEVELS, dtype=jnp.int32)
    out_pivots = out_pivots.at[kept].set(pivots[kept])
    out_links = out_links.at[kept].set(links[kept])
    out_logs = out_logs.at[kept].set(jax.vmap(final_block)(pivots[kept]))
    return (out_pivots, out_links, out_logs)
```

```python
import jax
import jax.numpy as jnp
from jax import lax
from jax.experimental import pallas as pl
from jax.experimental.pallas import tpu as pltpu
from jax.sharding import PartitionSpec as P

LEVELS = 4


def shifted(array, axis, by):
    devices = lax.axis_size(axis)
    pairs = [(i, i + by) for i in range(devices) if 0 <= i + by < devices]
    return lax.ppermute(array, axis, pairs)


LANES = 128
ROWS = 8


def hdot(left, right, dims=((1,), (0,))):
    return lax.dot_general(
        left, right, (dims, ((), ())), precision=lax.Precision.HIGHEST, preferred_element_type=jnp.float32
    )


def invert_lanes(block):
    sub = lax.broadcasted_iota(jnp.int32, (ROWS, LANES), 0)
    lane = lax.broadcasted_iota(jnp.int32, (ROWS, LANES), 1)
    strips = [block[ROWS * q : ROWS * (q + 1), :] for q in range(LANES // ROWS)]
    for p in range(len(strips)):
        base = ROWS * p
        spread = lambda strip: [
            jnp.broadcast_to(strip[:, base + j : base + j + 1], (ROWS, LANES)) for j in range(ROWS)
        ]
        inside = (lane >= base) & (lane < base + ROWS)
        panel = strips[p]
        cols = spread(panel)
        panel = jnp.where(inside, jnp.where(lane - base == sub, 1.0, 0.0), panel)
        for i in range(ROWS):
            here = sub == i
            scale = 1.0 / jnp.broadcast_to(cols[i][i : i + 1, :], (ROWS, LANES))
            factor = jnp.where(here, scale, -cols[i] * scale)
            panel = jnp.where(here, 0.0, panel) + factor * panel[i : i + 1, :]
            for j in range(i + 1, ROWS):
                cols[j] = jnp.where(here, 0.0, cols[j]) + factor * cols[j][i : i + 1, :]
        order = [q for q in range(p + 1, len(strips))] + [q for q in range(p)]
        for q in order:
            terms = [c * panel[j : j + 1, :] for j, c in enumerate(spread(strips[q]))]
            while len(terms) > 1:
                terms = [terms[m] + terms[m + 1] for m in range(0, len(terms), 2)]
            strips[q] = jnp.where(inside, 0.0, strips[q]) - terms[0]
        strips[p] = panel
    return jnp.concatenate(strips, axis=0)


def invert_ref(work):
    node_count = work.shape[0]

    def step(k, carry):
        here = pl.ds(pl.multiple_of(k * LANES, LANES), LANES)
        inverse = invert_lanes(work[here, here])
        solved = hdot(inverse, work[here, :])
        column = work[:, here]
        work[:, here] = jnp.zeros((node_count, LANES), jnp.float32)
        row_block = lax.broadcasted_iota(jnp.int32, (node_count, LANES), 0) // LANES
        column = jnp.where(row_block == k, 0.0, column)
        col_block = lax.broadcasted_iota(jnp.int32, (LANES, node_count), 1) // LANES
        wide = jnp.concatenate([inverse] * (node_count // LANES), axis=1)
        solved = jnp.where(col_block == k, wide, solved)
        work[...] = work[...] - hdot(column, solved)
        work[here, :] = solved
        return carry

    lax.fori_loop(0, node_count // LANES, step, 0)


def inverse_kernel(pivot_ref, inverse_ref):
    inverse_ref[...] = pivot_ref[...]
    invert_ref(inverse_ref)


def inverse_of(pivot):
    return pl.pallas_call(
        inverse_kernel,
        out_shape=jax.ShapeDtypeStruct(pivot.shape, jnp.float32),
        in_specs=[pl.BlockSpec(memory_space=pltpu.VMEM)],
        out_specs=pl.BlockSpec(memory_space=pltpu.VMEM),
    )(pivot)


def log_of(inverse, place):
    quarter = inverse.shape[0] // 4
    return lax.dynamic_slice_in_dim(jnp.log(jnp.diagonal(inverse)), place[2] * quarter, quarter, 0)


def whole_blocks(stacked):
    widened = lax.all_gather(stacked, "col", axis=2, tiled=True)
    return lax.all_gather(widened, "row", axis=1, tiled=True)


def send_later(gram_up, link_new, stride):
    return shifted((gram_up, link_new), "tm", stride)


def guarded(active, compute, zero_fill, operands):
    if active is None:
        return compute(operands)
    return lax.cond(active, compute, zero_fill, operands)


def half(array, index_id, axis):
    size = array.shape[axis] // 2
    return lax.dynamic_slice_in_dim(array, index_id * size, size, axis)


def eliminate_whole(operands, place):
    row_id, col_id, diag_id = place
    pivot, below, above = operands
    inverse = inverse_of(pivot)
    below_col = half(below, col_id, 1)
    above_row = half(above, row_id, 0)
    solved = hdot(inverse, below_col)
    gram_down = hdot(half(below, row_id, 1), solved, ((0,), (0,)))
    gram_up = hdot(above_row, hdot(inverse, half(above, col_id, 0), ((1,), (1,))))
    return (log_of(inverse, place), gram_down, gram_up, -hdot(above_row, solved))


def eliminate(pivot_tile, below_tile, above_tile, active, place):
    half_width = pivot_tile.shape[0]
    log_zero = jnp.zeros((half_width // 2,), jnp.float32)
    tile_zero = jnp.zeros((half_width, half_width), jnp.float32)
    whole = whole_blocks(jnp.stack([pivot_tile, below_tile, above_tile]))
    return guarded(
        active,
        lambda operands: eliminate_whole(operands, place),
        lambda operands: (log_zero, tile_zero, tile_zero, tile_zero),
        (whole[0], whole[1], whole[2]),
    )


def final_log(pivot, place):
    return log_of(inverse_of(pivot), place)


def shards(precision_diag, precision_link):
    row_id = lax.axis_index("row")
    col_id = lax.axis_index("col")
    time_id = lax.axis_index("tm")
    place = (row_id, col_id, row_id * 2 + col_id)
    device_count = lax.axis_size("tm")
    pivot_low = precision_diag[0]
    pivot_high = precision_diag[1]
    link_low = precision_link[0]
    link_high = jnp.where(
        time_id == device_count - 1, jnp.zeros_like(precision_link[1]), precision_link[1]
    )
    log_high, gram_down, gram_up, link_low = eliminate(pivot_high, link_low, link_high, None, place)
    ahead_gram, from_below = send_later(gram_up, link_low, 1)
    pivot_low = pivot_low - gram_down - ahead_gram
    log_low = jnp.zeros_like(log_high)
    for level_num in range(1, LEVELS):
        stride = 2 ** (level_num - 1)
        position = time_id % (2 * stride)
        active = position == stride
        keeper = position == 0
        below_link = from_below
        log_now, gram_down, gram_up, link_new = eliminate(
            pivot_low, below_link, link_low, active, place
        )
        back_gram, back_link = shifted((gram_down, link_new), "tm", -stride)
        ahead_gram, from_below = send_later(gram_up, link_new, stride)
        log_low = jnp.where(active, log_now, log_low)
        pivot_low = pivot_low - back_gram - ahead_gram
        link_low = jnp.where(keeper, back_link, link_low)
    remaining = time_id % 2 ** (LEVELS - 1) == 0
    whole_pivot = whole_blocks(pivot_low[None])[0]
    log_final = lax.cond(
        remaining,
        lambda pivot: final_log(pivot, place),
        lambda pivot: jnp.zeros_like(log_low),
        whole_pivot,
    )
    log_low = jnp.where(remaining, log_final, log_low)
    pivots = jnp.stack([pivot_low, pivot_high])
    couplings = jnp.stack([link_low, link_high])
    logs = jnp.stack([log_low, log_high])
    return (pivots, couplings, logs)


def solution(mesh):
    in_specs = (P("tm", "row", "col"), P("tm", "row", "col"))
    out_specs = (P("tm", "row", "col"), P("tm", "row", "col"), P("tm", ("row", "col")))
    return jax.shard_map(shards, mesh=mesh, in_specs=in_specs, out_specs=out_specs, check_vma=False)
```

```python
import jax
import jax.numpy as jnp
from jax import lax
from jax.experimental import pallas as pl
from jax.experimental.pallas import tpu as pltpu
from jax.sharding import PartitionSpec as P

LEVELS = 4

LANES = 128
ROWS = 8


def hdot(left, right, dims=((1,), (0,))):
    return lax.dot_general(
        left, right, (dims, ((), ())), precision=lax.Precision.HIGHEST, preferred_element_type=jnp.float32
    )


def invert_lanes(block):
    sub = lax.broadcasted_iota(jnp.int32, (ROWS, LANES), 0)
    lane = lax.broadcasted_iota(jnp.int32, (ROWS, LANES), 1)
    strips = [block[ROWS * q : ROWS * (q + 1), :] for q in range(LANES // ROWS)]
    for p in range(len(strips)):
        base = ROWS * p
        spread = lambda strip: [
            jnp.broadcast_to(strip[:, base + j : base + j + 1], (ROWS, LANES)) for j in range(ROWS)
        ]
        inside = (lane >= base) & (lane < base + ROWS)
        panel = strips[p]
        cols = spread(panel)
        panel = jnp.where(inside, jnp.where(lane - base == sub, 1.0, 0.0), panel)
        for i in range(ROWS):
            here = sub == i
            scale = 1.0 / jnp.broadcast_to(cols[i][i : i + 1, :], (ROWS, LANES))
            factor = jnp.where(here, scale, -cols[i] * scale)
            panel = jnp.where(here, 0.0, panel) + factor * panel[i : i + 1, :]
            for j in range(i + 1, ROWS):
                cols[j] = jnp.where(here, 0.0, cols[j]) + factor * cols[j][i : i + 1, :]
        order = [q for q in range(p + 1, len(strips))] + [q for q in range(p)]
        for q in order:
            terms = [c * panel[j : j + 1, :] for j, c in enumerate(spread(strips[q]))]
            while len(terms) > 1:
                terms = [terms[m] + terms[m + 1] for m in range(0, len(terms), 2)]
            strips[q] = jnp.where(inside, 0.0, strips[q]) - terms[0]
        strips[p] = panel
    return jnp.concatenate(strips, axis=0)


def invert_ref(work, between):
    node_count = work.shape[0]

    def step(k, carry):
        between(k)
        here = pl.ds(pl.multiple_of(k * LANES, LANES), LANES)
        inverse = invert_lanes(work[here, here])
        solved = hdot(inverse, work[here, :])
        column = work[:, here]
        work[:, here] = jnp.zeros((node_count, LANES), jnp.float32)
        row_block = lax.broadcasted_iota(jnp.int32, (node_count, LANES), 0) // LANES
        column = jnp.where(row_block == k, 0.0, column)
        col_block = lax.broadcasted_iota(jnp.int32, (LANES, node_count), 1) // LANES
        wide = jnp.concatenate([inverse] * (node_count // LANES), axis=1)
        solved = jnp.where(col_block == k, wide, solved)
        work[...] = work[...] - hdot(column, solved)
        work[here, :] = solved
        return carry

    lax.fori_loop(0, node_count // LANES, step, 0)


def cyclic_kernel(
    diag_ref, link_ref, pivot_ref, coupling_ref, log_ref,
    whole, work, made, ahead, back,
    x_send, x_recv, r_send, r_recv, f_send, f_recv,
    up_send, down_send, ahead_recv, back_recv,
):
    time_id, row_id, col_id = lax.axis_index("tm"), lax.axis_index("row"), lax.axis_index("col")
    times = lax.axis_size("tm")
    half = diag_ref.shape[1]
    node_count = 2 * half
    blocks = node_count // LANES
    reach = LEVELS - 1
    depth = sum((lax.rem(time_id, 2**j) == 0).astype(jnp.int32) for j in range(1, reach + 1))
    stride = sum(jnp.where(depth == j, 2**j, 0) for j in range(reach))
    mesh_id = pl.DeviceIdType.MESH

    def part(index):
        return pl.ds(pl.multiple_of(index * half, LANES), half)

    mine_rows, mine_cols = part(row_id), part(col_id)
    other_rows, other_cols = part(1 - row_id), part(1 - col_id)

    barrier = pltpu.get_barrier_semaphore()
    pl.semaphore_signal(barrier, inc=1, device_id={"col": 1 - col_id}, device_id_type=mesh_id)
    pl.semaphore_signal(barrier, inc=1, device_id={"row": 1 - row_id}, device_id_type=mesh_id)
    greeted = 2
    for j in range(reach):
        for by in (-(2**j), 2**j):
            near = (depth >= j) & (time_id + by >= 0) & (time_id + by < times)

            @pl.when(near)
            def _(by=by):
                pl.semaphore_signal(barrier, inc=1, device_id={"tm": time_id + by}, device_id_type=mesh_id)

            greeted = greeted + near.astype(jnp.int32)
    pl.semaphore_wait(barrier, greeted)

    def copy(src, dst, send, recv, target):
        return pltpu.make_async_remote_copy(
            src_ref=src, dst_ref=dst, send_sem=send, recv_sem=recv, device_id=target, device_id_type=mesh_id
        )

    def phase(ph, carry):
        first = ph == 0
        later = ph == 1
        solving = first | (depth < reach)
        on_diag = row_id == col_id

        def x_copy(a):
            tile = whole.at[ph, a, mine_rows, mine_cols]
            return copy(tile, tile, x_send.at[ph, a], x_recv.at[ph, a], {"col": 1 - col_id})

        def r_copy(a):
            tile = whole.at[ph, a, mine_rows, mine_cols]
            return copy(tile, tile, r_send.at[ph, a], r_recv.at[ph, a], {"row": 1 - row_id})

        def f_copy(a):
            tile = whole.at[ph, a, mine_rows, other_cols]
            return copy(tile, tile, f_send.at[ph, a], f_recv.at[ph, a], {"row": 1 - row_id})

        def up_copy(kind, source, level, by):
            return copy(
                made.at[ph, source], ahead.at[level, kind], up_send.at[ph, kind], ahead_recv.at[level, kind],
                {"tm": time_id + by},
            )

        def down_copy(kind, source, level, by):
            return copy(
                made.at[ph, source], back.at[level, kind], down_send.at[kind], back_recv.at[level, kind],
                {"tm": time_id - by},
            )

        def received(kind, level):
            by = 1 if level == 0 else 2 ** (level - 1)

            def from_below(use):
                @pl.when((depth >= level) & (time_id >= by))
                def _():
                    up_copy(kind, 0, level, 0).wait_recv()
                    use(ahead)

            def from_above(use):
                if level > 0:

                    @pl.when(depth >= level)
                    def _():
                        down_copy(kind, 0, level, 0).wait_recv()
                        use(back)

            return from_below, from_above

        @pl.when(first)
        def _():
            whole[0, 0, mine_rows, mine_cols] = diag_ref[1]
            pivot_ref[1] = diag_ref[1]
            high = jnp.where(time_id == times - 1, 0.0, link_ref[1])
            coupling_ref[1] = high
            whole[0, 1, mine_rows, mine_cols] = link_ref[0]
            whole[0, 2, mine_rows, mine_cols] = high

        @pl.when(later)
        def _():
            pivot_ref[0] = diag_ref[0] - made[0, 1]
            for level in range(LEVELS):
                def subtract(source, level=level):
                    pivot_ref[0] = pivot_ref[0] - source[level, 0]

                for arrival in received(0, level):
                    arrival(subtract)
            whole[1, 0, mine_rows, mine_cols] = pivot_ref[0]

        @pl.when(on_diag)
        def _():
            x_copy(0).start()

        r_copy(0).start()
        r_copy(0).wait_recv()

        @pl.when(jnp.logical_not(on_diag))
        def _():
            x_copy(0).wait_recv()
            f_copy(0).start()

        @pl.when(on_diag)
        def _():
            f_copy(0).wait_recv()

        work[:, mine_cols] = whole[ph, 0, :, mine_cols]
        far = part(1 - col_id)
        work[far, other_cols] = whole[ph, 0, far, other_cols]
        work[part(col_id), other_cols] = whole[ph, 0, far, mine_cols].T

        def between(k):
            @pl.when(k == 1)
            def _():
                @pl.when(later)
                def _():
                    coupling_ref[0] = made[0, 2]
                    for level in range(LEVELS):
                        def place_below(source, level=level):
                            whole[1, 1, mine_rows, mine_cols] = source[level, 1]

                        def place_above(source, level=level):
                            coupling_ref[0] = source[level, 1]

                        from_below, from_above = received(1, level)
                        from_below(place_below)
                        from_above(place_above)
                    whole[1, 2, mine_rows, mine_cols] = coupling_ref[0]

                @pl.when(solving)
                def _():
                    for a in (1, 2):
                        x_copy(a).start()
                        r_copy(a).start()

            @pl.when((k == blocks - 1) & solving)
            def _():
                for a in (1, 2):
                    x_copy(a).wait_recv()
                    f_copy(a).start()

        invert_ref(work, between)

        spot = pl.ds(pl.multiple_of((2 * row_id + col_id) * (node_count // 4), LANES), node_count // 4)
        corner = work[spot, spot]
        same = lax.broadcasted_iota(jnp.int32, corner.shape, 0) == lax.broadcasted_iota(jnp.int32, corner.shape, 1)
        log_ref[pl.ds(1 - ph, 1), :] = jnp.log(jnp.sum(jnp.where(same, corner, 0.0), axis=0, keepdims=True))

        @pl.when(solving)
        def _():
            for a in (1, 2):
                r_copy(a).wait_recv()
                f_copy(a).wait_recv()
            above_row = whole[ph, 2, mine_rows, :]
            level = jnp.where(first, 0, depth + 1)
            by = jnp.where(first, 1, stride)
            goes_up = time_id + by < times
            reached = hdot(work[...], whole[ph, 2, part(col_id), :], ((1,), (1,)))
            made[ph, 0] = hdot(above_row, reached)

            @pl.when(goes_up)
            def _():
                up_copy(0, 0, level, by).start()

            solved = hdot(work[...], whole[ph, 1, :, mine_cols])
            made[ph, 1] = hdot(whole[ph, 1, :, part(row_id)], solved, ((0,), (0,)))

            @pl.when(later)
            def _():
                down_copy(0, 1, level, by).start()

            made[ph, 2] = -hdot(above_row, solved)

            @pl.when(goes_up)
            def _():
                up_copy(1, 2, level, by).start()

            @pl.when(later)
            def _():
                down_copy(1, 2, level, by).start()

            for a in (1, 2):
                x_copy(a).wait_send()
                r_copy(a).wait_send()
                f_copy(a).wait_send()

        r_copy(0).wait_send()

        @pl.when(on_diag)
        def _():
            x_copy(0).wait_send()

        @pl.when(jnp.logical_not(on_diag))
        def _():
            f_copy(0).wait_send()

        @pl.when(later)
        def _():
            @pl.when(time_id + 1 < times)
            def _():
                for kind in (0, 1):
                    copy(
                        made.at[0, 2 * kind], ahead.at[0, kind], up_send.at[0, kind], ahead_recv.at[0, kind],
                        {"tm": time_id + 1},
                    ).wait_send()

            @pl.when(depth < reach)
            def _():
                for kind in (0, 1):
                    down_copy(kind, 1 + kind, depth + 1, stride).wait_send()

                    @pl.when(time_id + stride < times)
                    def _(kind=kind):
                        up_copy(kind, 2 * kind, depth + 1, stride).wait_send()

        return carry

    lax.fori_loop(0, 2, phase, 0)


def shards(precision_diag, precision_link):
    half = precision_diag.shape[1]
    node_count = 2 * half
    vmem = pl.BlockSpec(memory_space=pltpu.VMEM)
    dma = pltpu.SemaphoreType.DMA
    tile = (half, half)
    stack = jax.ShapeDtypeStruct(precision_diag.shape, jnp.float32)
    return pl.pallas_call(
        cyclic_kernel,
        out_shape=(stack, stack, jax.ShapeDtypeStruct((2, node_count // 4), jnp.float32)),
        in_specs=[vmem, vmem],
        out_specs=(vmem, vmem, vmem),
        scratch_shapes=[
            pltpu.VMEM((2, 3, node_count, node_count), jnp.float32),
            pltpu.VMEM((node_count, node_count), jnp.float32),
            pltpu.VMEM((2, 3) + tile, jnp.float32),
            pltpu.VMEM((LEVELS, 2) + tile, jnp.float32),
            pltpu.VMEM((LEVELS, 2) + tile, jnp.float32),
            dma((2, 3)), dma((2, 3)), dma((2, 3)), dma((2, 3)), dma((2, 3)), dma((2, 3)),
            dma((2, 2)), dma((2,)), dma((LEVELS, 2)), dma((LEVELS, 2)),
        ],
        compiler_params=pltpu.CompilerParams(collective_id=0, has_side_effects=True),
    )(precision_diag, precision_link)


def solution(mesh):
    in_specs = (P("tm", "row", "col"), P("tm", "row", "col"))
    out_specs = (P("tm", "row", "col"), P("tm", "row", "col"), P("tm", ("row", "col")))
    return jax.shard_map(shards, mesh=mesh, in_specs=in_specs, out_specs=out_specs, check_vma=False)
```

```python
import jax
import jax.numpy as jnp
from jax import lax
from jax.experimental import pallas as pl
from jax.experimental.pallas import tpu as pltpu
from jax.sharding import PartitionSpec as P

LEVELS = 4

LANES = 128
ROWS = 8
GROUP = 32


def hdot(left, right, dims=((1,), (0,))):
    return lax.dot_general(
        left, right, (dims, ((), ())), precision=lax.Precision.HIGHEST, preferred_element_type=jnp.float32
    )


def split_three(array):
    high = array.astype(jnp.bfloat16)
    rest = array - high.astype(jnp.float32)
    middle = rest.astype(jnp.bfloat16)
    return high, middle, (rest - middle.astype(jnp.float32)).astype(jnp.bfloat16)


def packed_dot(left, right):
    high, middle, low = split_three(left)
    first, second, third = split_three(right)
    wide = jnp.concatenate([high, high, middle, middle, high, low], axis=1)
    tall = jnp.concatenate([first, second, first, second, third, first], axis=0)
    return jnp.dot(wide, tall, preferred_element_type=jnp.float32)


def sweep_group(strips, start):
    sub = lax.broadcasted_iota(jnp.int32, (ROWS, LANES), 0)
    lane = lax.broadcasted_iota(jnp.int32, (ROWS, LANES), 1)
    pick = lambda strip, row: jnp.broadcast_to(strip[row : row + 1, :], (ROWS, LANES))
    strips = list(strips)
    count = len(strips)

    def spread(strip, p):
        return [
            jnp.broadcast_to(strip[:, start + ROWS * p + j : start + ROWS * p + j + 1], (ROWS, LANES)) for j in range(ROWS)
        ]

    def total(terms):
        while len(terms) > 1:
            terms = [terms[m] + terms[m + 1] for m in range(0, len(terms), 2)]
        return terms[0]

    cols = spread(strips[0], 0)
    for p in range(count):
        base = start + ROWS * p
        inside = (lane >= base) & (lane < base + ROWS)
        panel = jnp.where(inside, jnp.where(lane - base == sub, 1.0, 0.0), strips[p])
        if p + 1 < count:
            ahead_cols = spread(strips[p], p + 1)
            next_left = spread(strips[p + 1], p)
            next_cols = spread(strips[p + 1], p + 1)
        for i in range(0, ROWS, 2):
            first, second = cols[i], cols[i + 1]
            on_first, on_second = sub == i, sub == i + 1
            outside = (sub < i) | (sub > i + 1)
            a, b = pick(first, i), pick(first, i + 1)
            d = pick(second, i + 1)
            det = a * d - b * b
            scale = pl.reciprocal(det, approx=True)
            left = jnp.where(on_first, d, jnp.where(on_second, -b, second * b - first * d))
            right = jnp.where(on_second, a, jnp.where(on_first, -b, first * b - second * a))
            scale = scale * (2.0 - det * scale)
            apply = lambda strip: jnp.where(outside, strip, 0.0) + scale * (left * pick(strip, i) + right * pick(strip, i + 1))
            panel = apply(panel)
            for j in range(i + 2, ROWS):
                cols[j] = apply(cols[j])
            if p + 1 < count:
                ahead_cols = [apply(strip) for strip in ahead_cols]
        if p + 1 < count:
            cols = [
                next_cols[j] - total([next_left[m] * pick(ahead_cols[j], m) for m in range(ROWS)])
                for j in range(ROWS)
            ]
        for q in [q for q in range(p + 1, count)] + [q for q in range(p)]:
            left_cols = next_left if q == p + 1 else spread(strips[q], p)
            strips[q] = jnp.where(inside, 0.0, strips[q]) - total(
                [c * pick(panel, j) for j, c in enumerate(left_cols)]
            )
        strips[p] = panel
    return strips


def invert_lanes(block):
    lane = lax.broadcasted_iota(jnp.int32, (LANES, LANES), 1)
    for start in range(0, LANES, GROUP):
        strips = [block[start + ROWS * q : start + ROWS * (q + 1), :] for q in range(GROUP // ROWS)]
        solved = sweep_group(strips, start)
        inside = (lane >= start) & (lane < start + GROUP)
        above = [jnp.zeros((start, LANES), jnp.float32)] if start else []
        rest = LANES - start - GROUP
        below = [jnp.zeros((rest, LANES), jnp.float32)] if rest else []
        padded = jnp.concatenate(above + solved + below, axis=0)
        update = packed_dot(jnp.where(inside, block, 0.0), padded)
        block = jnp.where(inside, 0.0, block) - update
        block = jnp.concatenate(
            ([block[:start, :]] if start else []) + solved + ([block[start + GROUP :, :]] if rest else []), axis=0
        )
    return block


def invert_ref(work, between, first_block=0):
    node_count = work.shape[0]

    def step(k, carry):
        between(k)
        block_id = lax.rem(k + first_block, node_count // LANES)
        here = pl.ds(pl.multiple_of(block_id * LANES, LANES), LANES)
        inverse = invert_lanes(work[here, here])
        solved = packed_dot(inverse, work[here, :])
        column = work[:, here]
        work[:, here] = jnp.zeros((node_count, LANES), jnp.float32)
        row_block = lax.broadcasted_iota(jnp.int32, (node_count, LANES), 0) // LANES
        column = jnp.where(row_block == block_id, 0.0, column)
        col_block = lax.broadcasted_iota(jnp.int32, (LANES, node_count), 1) // LANES
        wide = jnp.concatenate([inverse] * (node_count // LANES), axis=1)
        solved = jnp.where(col_block == block_id, wide, solved)
        work[...] = work[...] - packed_dot(column, solved)
        work[here, :] = solved
        return carry

    lax.fori_loop(0, node_count // LANES, step, 0)


def cyclic_kernel(
    diag_ref, link_ref, pivot_ref, coupling_ref, log_ref,
    whole, work, made, ahead, back,
    x_send, x_recv, r_send, r_recv, f_send, f_recv,
    up_send, down_send, ahead_recv, back_recv,
):
    time_id, row_id, col_id = lax.axis_index("tm"), lax.axis_index("row"), lax.axis_index("col")
    times = lax.axis_size("tm")
    half = diag_ref.shape[1]
    node_count = 2 * half
    blocks = node_count // LANES
    reach = LEVELS - 1
    depth = sum((lax.rem(time_id, 2**j) == 0).astype(jnp.int32) for j in range(1, reach + 1))
    stride = sum(jnp.where(depth == j, 2**j, 0) for j in range(reach))
    mesh_id = pl.DeviceIdType.MESH

    def part(index):
        return pl.ds(pl.multiple_of(index * half, LANES), half)

    mine_rows, mine_cols = part(row_id), part(col_id)
    other_rows, other_cols = part(1 - row_id), part(1 - col_id)

    barrier = pltpu.get_barrier_semaphore()
    pl.semaphore_signal(barrier, inc=1, device_id={"col": 1 - col_id}, device_id_type=mesh_id)
    pl.semaphore_signal(barrier, inc=1, device_id={"row": 1 - row_id}, device_id_type=mesh_id)
    greeted = 2
    for j in range(reach):
        for by in (-(2**j), 2**j):
            near = (depth >= j) & (time_id + by >= 0) & (time_id + by < times)

            @pl.when(near)
            def _(by=by):
                pl.semaphore_signal(barrier, inc=1, device_id={"tm": time_id + by}, device_id_type=mesh_id)

            greeted = greeted + near.astype(jnp.int32)
    pl.semaphore_wait(barrier, greeted)

    def copy(src, dst, send, recv, target):
        return pltpu.make_async_remote_copy(
            src_ref=src, dst_ref=dst, send_sem=send, recv_sem=recv, device_id=target, device_id_type=mesh_id
        )

    def phase(ph, carry):
        first = ph == 0
        later = ph == 1
        solving = first | (depth < reach)
        on_diag = row_id == col_id

        def x_copy(a):
            tile = whole.at[ph, a, mine_rows, mine_cols]
            return copy(tile, tile, x_send.at[ph, a], x_recv.at[ph, a], {"col": 1 - col_id})

        def r_copy(a):
            tile = whole.at[ph, a, mine_rows, mine_cols]
            return copy(tile, tile, r_send.at[ph, a], r_recv.at[ph, a], {"row": 1 - row_id})

        def f_copy(a):
            tile = whole.at[ph, a, mine_rows, other_cols]
            return copy(tile, tile, f_send.at[ph, a], f_recv.at[ph, a], {"row": 1 - row_id})

        def up_copy(kind, source, level, by):
            return copy(
                made.at[ph, source], ahead.at[level, kind], up_send.at[ph, kind], ahead_recv.at[level, kind],
                {"tm": time_id + by},
            )

        def down_copy(kind, source, level, by):
            return copy(
                made.at[ph, source], back.at[level, kind], down_send.at[kind], back_recv.at[level, kind],
                {"tm": time_id - by},
            )

        def received(kind, level):
            by = 1 if level == 0 else 2 ** (level - 1)

            def from_below(use):
                @pl.when((depth >= level) & (time_id >= by))
                def _():
                    up_copy(kind, 0, level, 0).wait_recv()
                    use(ahead)

            def from_above(use):
                if level > 0:

                    @pl.when(depth >= level)
                    def _():
                        down_copy(kind, 0, level, 0).wait_recv()
                        use(back)

            return from_below, from_above

        @pl.when(first)
        def _():
            whole[0, 0, mine_rows, mine_cols] = diag_ref[1]
            pivot_ref[1] = diag_ref[1]
            high = jnp.where(time_id == times - 1, 0.0, link_ref[1])
            coupling_ref[1] = high
            whole[0, 1, mine_rows, mine_cols] = link_ref[0]
            whole[0, 2, mine_rows, mine_cols] = high

        @pl.when(later)
        def _():
            pivot_ref[0] = diag_ref[0] - made[0, 1]
            for level in range(LEVELS):
                def subtract(source, level=level):
                    pivot_ref[0] = pivot_ref[0] - source[level, 0]

                for arrival in received(0, level):
                    arrival(subtract)
            whole[1, 0, mine_rows, mine_cols] = pivot_ref[0]

        @pl.when(on_diag)
        def _():
            x_copy(0).start()

        r_copy(0).start()
        r_copy(0).wait_recv()

        work[:, mine_cols] = whole[ph, 0, :, mine_cols]
        far = part(1 - col_id)
        work[far, other_cols] = jnp.zeros((half, half), jnp.float32)
        work[part(col_id), other_cols] = whole[ph, 0, far, mine_cols].T

        def between(k):
            @pl.when((k == 1) & jnp.logical_not(on_diag))
            def _():
                x_copy(0).wait_recv()
                f_copy(0).start()

            @pl.when(k == blocks // 2)
            def _():
                @pl.when(on_diag)
                def _():
                    f_copy(0).wait_recv()

                work[far, other_cols] = work[far, other_cols] + whole[ph, 0, far, other_cols]

            @pl.when(k == jnp.where(first, 0, 1))
            def _():
                @pl.when(later)
                def _():
                    coupling_ref[0] = made[0, 2]
                    for level in range(LEVELS):
                        def place_below(source, level=level):
                            whole[1, 1, mine_rows, mine_cols] = source[level, 1]

                        def place_above(source, level=level):
                            coupling_ref[0] = source[level, 1]

                        from_below, from_above = received(1, level)
                        from_below(place_below)
                        from_above(place_above)
                    whole[1, 2, mine_rows, mine_cols] = coupling_ref[0]

                @pl.when(solving)
                def _():
                    for a in (2, 1):
                        x_copy(a).start()
                        r_copy(a).start()

            @pl.when((k == blocks - 1) & solving)
            def _():
                x_copy(2).wait_recv()
                f_copy(2).start()

        invert_ref(work, between, col_id * (blocks // 2))

        spot = pl.ds(pl.multiple_of((2 * row_id + col_id) * (node_count // 4), LANES), node_count // 4)
        corner = work[spot, spot]
        same = lax.broadcasted_iota(jnp.int32, corner.shape, 0) == lax.broadcasted_iota(jnp.int32, corner.shape, 1)
        log_ref[pl.ds(1 - ph, 1), :] = jnp.log(jnp.sum(jnp.where(same, corner, 0.0), axis=0, keepdims=True))

        @pl.when(solving)
        def _():
            x_copy(1).wait_recv()
            f_copy(1).start()
            r_copy(2).wait_recv()
            f_copy(2).wait_recv()
            above_row = whole[ph, 2, mine_rows, :]
            level = jnp.where(first, 0, depth + 1)
            by = jnp.where(first, 1, stride)
            goes_up = time_id + by < times
            reached = hdot(work[...], whole[ph, 2, part(col_id), :], ((1,), (1,)))
            made[ph, 0] = hdot(above_row, reached)

            @pl.when(goes_up)
            def _():
                up_copy(0, 0, level, by).start()

            r_copy(1).wait_recv()
            solved = hdot(work[...], whole[ph, 1, :, mine_cols])
            f_copy(1).wait_recv()
            made[ph, 1] = hdot(whole[ph, 1, :, part(row_id)], solved, ((0,), (0,)))

            @pl.when(later)
            def _():
                down_copy(0, 1, level, by).start()

            made[ph, 2] = -hdot(above_row, solved)

            @pl.when(goes_up)
            def _():
                up_copy(1, 2, level, by).start()

            @pl.when(later)
            def _():
                down_copy(1, 2, level, by).start()

            for a in (1, 2):
                x_copy(a).wait_send()
                r_copy(a).wait_send()
                f_copy(a).wait_send()

        r_copy(0).wait_send()

        @pl.when(on_diag)
        def _():
            x_copy(0).wait_send()

        @pl.when(jnp.logical_not(on_diag))
        def _():
            f_copy(0).wait_send()

        @pl.when(later)
        def _():
            @pl.when(time_id + 1 < times)
            def _():
                for kind in (0, 1):
                    copy(
                        made.at[0, 2 * kind], ahead.at[0, kind], up_send.at[0, kind], ahead_recv.at[0, kind],
                        {"tm": time_id + 1},
                    ).wait_send()

            @pl.when(depth < reach)
            def _():
                for kind in (0, 1):
                    down_copy(kind, 1 + kind, depth + 1, stride).wait_send()

                    @pl.when(time_id + stride < times)
                    def _(kind=kind):
                        up_copy(kind, 2 * kind, depth + 1, stride).wait_send()

        return carry

    lax.fori_loop(0, 2, phase, 0)


def shards(precision_diag, precision_link):
    half = precision_diag.shape[1]
    node_count = 2 * half
    vmem = pl.BlockSpec(memory_space=pltpu.VMEM)
    dma = pltpu.SemaphoreType.DMA
    tile = (half, half)
    stack = jax.ShapeDtypeStruct(precision_diag.shape, jnp.float32)
    return pl.pallas_call(
        cyclic_kernel,
        out_shape=(stack, stack, jax.ShapeDtypeStruct((2, node_count // 4), jnp.float32)),
        in_specs=[vmem, vmem],
        out_specs=(vmem, vmem, vmem),
        scratch_shapes=[
            pltpu.VMEM((2, 3, node_count, node_count), jnp.float32),
            pltpu.VMEM((node_count, node_count), jnp.float32),
            pltpu.VMEM((2, 3) + tile, jnp.float32),
            pltpu.VMEM((LEVELS, 2) + tile, jnp.float32),
            pltpu.VMEM((LEVELS, 2) + tile, jnp.float32),
            dma((2, 3)), dma((2, 3)), dma((2, 3)), dma((2, 3)), dma((2, 3)), dma((2, 3)),
            dma((2, 2)), dma((2,)), dma((LEVELS, 2)), dma((LEVELS, 2)),
        ],
        compiler_params=pltpu.CompilerParams(collective_id=0, has_side_effects=True),
    )(precision_diag, precision_link)


def solution(mesh):
    in_specs = (P("tm", "row", "col"), P("tm", "row", "col"))
    out_specs = (P("tm", "row", "col"), P("tm", "row", "col"), P("tm", ("row", "col")))
    return jax.shard_map(shards, mesh=mesh, in_specs=in_specs, out_specs=out_specs, check_vma=False)
```
